256 devices in a mesh: ia: 16 (over y, x_hi, core), ja: 8 (over z), af: 2 (over x_lo).
Axes of the slice: x: 4 (x_hi: 2, x_lo: 2; x = x_hi * 2 + x_lo), y: 4, z: 8, core: 2. Of those that a mesh axis runs over, the one named last changes fastest.
Arguments:
- alleles: int32 [2048, 1024], P(('ia', 'ja'), 'af'), may hold values from -2147483648 to 2147483646
- section: int32 [1], replicated, may hold values from 0 to 255
Outputs:
- metric: float32 [8, 2048, 2048], P('af', 'ia', 'ja')
The draws below stay inside these ranges and needn't reach their ends.
Inputs may be any that keep to these rules, and one draw needn't show every extreme that they name: `section`: the slab of third vectors lies inside the vector range.
All inputs are finite; a program needn't handle non-finite values.
Results may differ from the reference program's by a relative error of at most 0.0003.
Values sent between devices are 32-bit elements; how exact they have to be, the bound alone decides.
No kernel may reach another device: no remote copies, remote signals or barrier semaphores. Data moves between devices by JAX's collectives and lax.ppermute only.
A program may use at most 64 MiB of HBM per device.

```python
import jax
import jax.numpy as jnp
from jax import lax

KS = 8
NV = 2048
NW = 1024


def touch_ends(result, rng, least, high):
    place = [jax.random.randint(jax.random.fold_in(rng, axis), (), 0, length) for axis, length in enumerate(result.shape)]
    longest = result.shape.index(max(result.shape))
    neighbour = place[:longest] + [(place[longest] + 1) % result.shape[longest]] + place[longest + 1:]
    return result.at[tuple(place)].set(least).at[tuple(neighbour)].set(high)


def setup_inputs(seed: int = 0) -> dict:
    streams_of = jax.random.split(jax.random.key(seed), 3)
    return {
        "alleles": touch_ends(jax.random.randint(streams_of[0], (NV, NW), -2147483648, 2147483647), jax.random.fold_in(streams_of[0], 1), -2147483648, 2147483646).astype(jnp.int32),
        "section": jax.random.randint(streams_of[1], (1,), 0, NV // KS).astype(jnp.int32),
    }


def unpack_rows(words):
    shifts = 2 * jnp.arange(16, dtype=jnp.int32)
    fields = jnp.bitwise_and(jnp.right_shift(words[:, :, None], shifts), 3)
    low_bit = jnp.bitwise_and(fields, 1)
    high_bit = jnp.right_shift(fields, 1)
    row_count = words.shape[0]
    bit_rows = jnp.stack([low_bit.reshape(row_count, -1), high_bit.reshape(row_count, -1)], axis=1).reshape(row_count, -1)
    ones_count = jnp.sum(low_bit + high_bit, axis=(1, 2)).astype(jnp.float32)
    return bit_rows.astype(jnp.float32), ones_count


def reference(alleles, section):
    bit_rows, ones_count = unpack_rows(alleles)
    offset_row = (section[0] * KS).astype(jnp.int32)
    third_bits = lax.dynamic_slice_in_dim(bit_rows, offset_row, KS, 0)
    third_ones = lax.dynamic_slice_in_dim(ones_count, offset_row, KS, 0)

    def one_third(third_row):
        product_rows = bit_rows * third_row[None, :]
        return lax.dot_general(product_rows, bit_rows, (((1,), (1,)), ((), ())), preferred_element_type=jnp.float32)

    counts = lax.map(one_third, third_bits)
    denominator = third_ones[:, None, None] + ones_count[None, :, None] + ones_count[None, None, :] + 1.0
    return 3.0 * counts / denominator
```

```python
import jax
import jax.numpy as jnp
from jax import lax
from jax.experimental import pallas as pl
from jax.experimental.pallas import tpu as pltpu
from jax.sharding import Mesh
from jax.sharding import PartitionSpec as P

KS = 8
ROWS = 16
SIDE = ("y", "xh")
PLACES = {4: (0, 0), 3: (1, 0), 5: (3, 0), 2: (2, 0), 6: (0, 1), 1: (1, 1), 7: (3, 1), 0: (2, 1)}


def broadcast_all(array, axis):
    size = lax.axis_size(axis)
    return lax.all_to_all(
        jnp.broadcast_to(array[None], (size, *array.shape)), axis, 0, 0, tiled=True
    )


def to_planes(array):
    pairs = []
    for y in range(4):
        for xh in range(2):
            for c in range(2):
                for z in range(8):
                    plane = 2 * y + xh
                    dy, dx = PLACES[(z - plane) % 8]
                    there = (((y + dy) % 4) * 2 + (xh + dx) % 2) * 2 + c
                    pairs.append((((y * 2 + xh) * 2 + c) * 8 + z, there * 8 + plane))
    return lax.ppermute(array, ("y", "xh", "c", "z"), pairs)


def swap(array, axis):
    return lax.ppermute(array, axis, [(0, 1), (1, 0)])


def place_j(scal, mine, theirs, jbuf):
    core = scal[0]
    plane = scal[1]
    base_y, base_x = plane // 2, plane % 2
    for dz, (dy, dx) in PLACES.items():
        slot = lax.rem(base_y + dy, 4) * 2 + lax.rem(base_x + dx, 2)
        row = lax.rem(plane + dz, 8) * ROWS
        src = pl.multiple_of(slot * ROWS, ROWS)
        own = pl.multiple_of(core * 128 + row, ROWS)
        other = pl.multiple_of((1 - core) * 128 + row, ROWS)
        jbuf[pl.ds(own, ROWS), :] = mine[pl.ds(src, ROWS), :]
        jbuf[pl.ds(other, ROWS), :] = theirs[pl.ds(src, ROWS), :]


def third_rows(scal, mine, theirs):
    at = pl.multiple_of(128 + 4 * 0, 8)
    slab = jnp.where(scal[2] == scal[0], mine[pl.ds(at, KS), :], theirs[pl.ds(at, KS), :])
    return jnp.where(scal[3] == 0, slab[0:4], slab[4:8])


BITS = 4


def accumulate(iw_ref, jbuf, kw, acc_ref, first):
    for g in range(32 // BITS):
        lhs, rhs = [], []
        for bit in range(g * BITS, (g + 1) * BITS):
            mask = jnp.int32((1 << bit) - (1 << 32 if bit == 31 else 0))
            i_bits = (iw_ref[...] & mask).astype(jnp.float32).astype(jnp.bfloat16)
            j_bits = (jbuf[...] & mask).astype(jnp.float32).astype(jnp.bfloat16)
            k_bits = ((lax.shift_right_logical(kw, bit) & 1).astype(jnp.float32) * (2.0 ** (-2 * bit))).astype(
                jnp.bfloat16
            )
            lhs.append(jnp.concatenate([i_bits * k_bits[t : t + 1] for t in range(4)], axis=0))
            rhs.append(j_bits)
        part = lax.dot_general(
            jnp.concatenate(lhs, axis=1),
            jnp.concatenate(rhs, axis=1),
            (((1,), (1,)), ((), ())),
            preferred_element_type=jnp.float32,
        )
        if g == 0 and first:
            acc_ref[...] = part
        else:
            acc_ref[...] += part


def half_kernel(scal, iw, mine, theirs, acc, jbuf):
    place_j(scal, mine, theirs, jbuf)
    accumulate(iw, jbuf, third_rows(scal, mine, theirs), acc, True)


def popcounts(words):
    return lax.population_count(words).astype(jnp.float32)


def last_kernel(scal, iw0, iw, mine0, theirs0, mine, theirs, partial, out, jbuf0, jbuf, acc):
    place_j(scal, mine0, theirs0, jbuf0)
    place_j(scal, mine, theirs, jbuf)
    acc[...] = partial[...]
    kw0 = third_rows(scal, mine0, theirs0)
    kw = third_rows(scal, mine, theirs)
    accumulate(iw, jbuf, kw, acc, False)
    ones_i = jnp.sum(popcounts(iw0[...]) + popcounts(iw[...]), axis=1, keepdims=True)
    ones_k = jnp.sum(popcounts(kw0) + popcounts(kw), axis=1, keepdims=True)
    j_counts = (popcounts(jbuf0[...]) + popcounts(jbuf[...])).astype(jnp.bfloat16)
    ones_j = lax.dot_general(
        jnp.ones((8, j_counts.shape[1]), jnp.bfloat16),
        j_counts,
        (((1,), (1,)), ((), ())),
        preferred_element_type=jnp.float32,
    )[0:1]
    for t in range(4):
        denominator = ones_k[t : t + 1] + ones_i + ones_j + 1.0
        out[t] = 3.0 * acc[t * 128 : (t + 1) * 128, :] / denominator


VM = pl.BlockSpec(memory_space=pltpu.VMEM)
SM = pl.BlockSpec(memory_space=pltpu.SMEM)
COST = pl.CostEstimate(flops=2 * 512 * 256 * 16384, bytes_accessed=2**20, transcendentals=0)


def per_device(alleles, section):
    core = lax.axis_index("c")
    plane = lax.axis_index("z")
    words = alleles.shape[1]
    row = section[0] * KS
    ia_s = row // 128
    moved = to_planes(alleles)
    iwords = broadcast_all(alleles, "z").reshape(128, words)
    iother = swap(iwords, "xl")
    slab = lax.dynamic_slice_in_dim(iwords, lax.rem(row, 128), KS, 0)
    got = broadcast_all(jnp.concatenate([moved, slab], axis=0), SIDE)
    k_mine = lax.dynamic_index_in_dim(got, ia_s // 2, 0, keepdims=False)[ROWS:]
    mine = jnp.concatenate([got[:, :ROWS].reshape(128, words), k_mine], axis=0)
    mine_x = swap(mine, "xl")
    theirs = swap(mine, "c")
    scal = jnp.stack([core, plane, lax.rem(ia_s, 2), lax.axis_index("xl")]).astype(jnp.int32)
    partial = pl.pallas_call(
        half_kernel,
        out_shape=jax.ShapeDtypeStruct((512, 256), jnp.float32),
        in_specs=[SM, VM, VM, VM],
        out_specs=VM,
        scratch_shapes=[pltpu.VMEM((256, words), jnp.int32)],
        cost_estimate=COST,
        name="own_half",
    )(scal, iwords, mine, theirs)
    theirs_x = swap(mine_x, "c")
    return pl.pallas_call(
        last_kernel,
        out_shape=jax.ShapeDtypeStruct((4, 128, 256), jnp.float32),
        in_specs=[SM] + [VM] * 7,
        out_specs=VM,
        scratch_shapes=[
            pltpu.VMEM((256, words), jnp.int32),
            pltpu.VMEM((256, words), jnp.int32),
            pltpu.VMEM((512, 256), jnp.float32),
        ],
        cost_estimate=COST,
        name="other_half",
    )(scal, iwords, iother, mine, theirs, mine_x, theirs_x, partial)


def solution(mesh):
    torus = Mesh(
        mesh.devices.reshape(4, 2, 2, mesh.shape["ja"], mesh.shape["af"]),
        ("y", "xh", "c", "z", "xl"),
    )
    in_specs = (P(("y", "xh", "c", "z"), "xl"), P())
    out_specs = P("xl", ("y", "xh", "c"), "z")
    return jax.shard_map(
        per_device, mesh=torus, in_specs=in_specs, out_specs=out_specs, check_vma=False
    )
```

```python
import jax
import jax.numpy as jnp
from jax import lax
from jax.experimental import pallas as pl
from jax.experimental.pallas import tpu as pltpu
from jax.sharding import Mesh
from jax.sharding import PartitionSpec as P

KS = 8
ROWS = 16
F8 = jnp.float8_e4m3fn
PLACES = {4: (0, 0), 3: (1, 0), 5: (3, 0), 2: (2, 0), 6: (0, 1), 1: (1, 1), 7: (3, 1), 0: (2, 1)}
Y_STEPS = (0, 1, 3, 2)


def broadcast_all(array, axis):
    size = lax.axis_size(axis)
    return lax.all_to_all(
        jnp.broadcast_to(array[None], (size, *array.shape)), axis, 0, 0, tiled=True
    )


def to_planes(array):
    pairs = []
    for y in range(4):
        for xh in range(2):
            for c in range(2):
                for z in range(8):
                    plane = 2 * y + xh
                    dy, dx = PLACES[(z - plane) % 8]
                    there = (((y + dy) % 4) * 2 + (xh + dx) % 2) * 2 + c
                    pairs.append((((y * 2 + xh) * 2 + c) * 8 + z, there * 8 + plane))
    return lax.ppermute(array, ("y", "xh", "c", "z"), pairs)


def swap(array, axis, bit=1):
    return lax.ppermute(array, axis, [(n, n ^ bit) for n in range(lax.axis_size(axis))])


def spread(array, axis, bit, root):
    other = swap(array, axis, bit)
    return jnp.where((lax.axis_index(axis) & bit) == (root & bit), array, other)


def bits(words, bit):
    mask = jnp.int8((1 << bit) - (1 << 8 if bit == 7 else 0))
    return jnp.where((words & mask) != 0, jnp.full(words.shape, 1, F8), jnp.full(words.shape, 0, F8))


def pieces(words):
    return [(lax.shift_right_logical(words, s) if s else words).astype(jnp.int8) for s in range(0, 32, 8)]


def popcounts(words):
    return lax.population_count(words).astype(jnp.float32)


def place_j(scal, mine, theirs, jbuf):
    core, plane, y, xh = scal[0], scal[1], scal[2], scal[3]
    for slot in range(8):
        y_from = y - Y_STEPS[slot // 2]
        dy = (y_from - plane // 2) & 3
        dx = (xh + slot + plane) & 1
        dz = jnp.int32(0)
        for step, (at_y, at_x) in PLACES.items():
            dz = jnp.where((dy == at_y) & (dx == at_x), step, dz)
        row = ((plane + dz) & 7) * ROWS
        own = pl.multiple_of(core * 128 + row, ROWS)
        other = pl.multiple_of((1 - core) * 128 + row, ROWS)
        jbuf[pl.ds(own, ROWS), :] = mine[slot * ROWS : (slot + 1) * ROWS, :]
        jbuf[pl.ds(other, ROWS), :] = theirs[slot * ROWS : (slot + 1) * ROWS, :]


def kernel(scal, iw, iw_x, mine, theirs, mine_x, theirs_x, thirds, out, jbuf, jbuf_x, acc):
    place_j(scal, mine, theirs, jbuf)
    place_j(scal, mine_x, theirs_x, jbuf_x)
    first = True
    for half, (i_ref, j_ref) in enumerate(((iw, jbuf), (iw_x, jbuf_x))):
        i_parts, j_parts = pieces(i_ref[...]), pieces(j_ref[...])
        k_parts = pieces(thirds[4 * half : 4 * half + 4])
        for i_part, j_part, k_part in zip(i_parts, j_parts, k_parts):
            pairs = jnp.concatenate([i_part & k_part[t : t + 1] for t in range(4)], axis=0)
            part = lax.dot_general(
                jnp.concatenate([bits(pairs, b) for b in range(8)], axis=1),
                jnp.concatenate([bits(j_part, b) for b in range(8)], axis=1),
                (((1,), (1,)), ((), ())),
                preferred_element_type=jnp.float32,
            )
            acc[...] = part if first else acc[...] + part
            first = False
    ones_i = jnp.sum(popcounts(iw[...]) + popcounts(iw_x[...]), axis=1, keepdims=True)
    ones_k = jnp.sum(popcounts(thirds[0:4]) + popcounts(thirds[4:8]), axis=1, keepdims=True)
    j_counts = (popcounts(jbuf[...]) + popcounts(jbuf_x[...])).astype(jnp.bfloat16)
    ones_j = lax.dot_general(
        jnp.ones((8, j_counts.shape[1]), jnp.bfloat16),
        j_counts,
        (((1,), (1,)), ((), ())),
        preferred_element_type=jnp.float32,
    )[0:1]
    for t in range(4):
        denominator = ones_k[t : t + 1] + ones_i + ones_j + 1.0
        out[t] = 3.0 * acc[t * 128 : (t + 1) * 128, :] / denominator


VM = pl.BlockSpec(memory_space=pltpu.VMEM)
SM = pl.BlockSpec(memory_space=pltpu.SMEM)
COST = pl.CostEstimate(flops=2 * 512 * 256 * 32768, bytes_accessed=2**21, transcendentals=0)
IN_VMEM = True


def per_device(alleles, section):
    words = alleles.shape[1]
    half = lax.axis_index("xl")
    row = section[0] * KS
    ia_s = row // 128
    scal = jnp.stack([lax.axis_index(a) for a in ("c", "z", "y", "xh")]).astype(jnp.int32)
    moved = to_planes(alleles)
    iwords = broadcast_all(alleles, "z").reshape(128, words)
    pair = jnp.concatenate([moved, swap(moved, "xh")], axis=0)
    turns = [lax.ppermute(pair, "y", [(n, (n + d) % 4) for n in range(4)]) for d in Y_STEPS[1:]]
    mine = jnp.concatenate([pair, *turns], axis=0)
    at = lax.rem(row, 128)
    k_own = lax.dynamic_slice_in_dim(iwords, at + 4 * half, 4, 0)
    k_send = lax.dynamic_slice_in_dim(iwords, at + 4 * (1 - half), 4, 0)
    thirds = jnp.concatenate([k_own, swap(k_send, "xl")], axis=0)
    thirds = spread(thirds, "c", 1, lax.rem(ia_s, 2))
    thirds = spread(thirds, "xh", 1, lax.rem(ia_s // 2, 2))
    thirds = spread(thirds, "y", 1, ia_s // 4)
    thirds = spread(thirds, "y", 2, ia_s // 4)
    iwords_x = swap(iwords, "xl")
    mine_x = swap(mine, "xl")
    theirs = swap(mine, "c")
    theirs_x = swap(mine_x, "c")
    operands = [iwords, iwords_x, mine, theirs, mine_x, theirs_x, thirds]
    if IN_VMEM:
        operands = [pltpu.with_memory_space_constraint(a, pltpu.VMEM) for a in operands]
    return pl.pallas_call(
        kernel,
        out_shape=jax.ShapeDtypeStruct((4, 128, 256), jnp.float32),
        in_specs=[SM] + [VM] * 7,
        out_specs=VM,
        scratch_shapes=[
            pltpu.VMEM((256, words), jnp.int32),
            pltpu.VMEM((256, words), jnp.int32),
            pltpu.VMEM((512, 256), jnp.float32),
        ],
        cost_estimate=COST,
        name="metric",
    )(scal, *operands)


def solution(mesh):
    torus = Mesh(
        mesh.devices.reshape(4, 2, 2, mesh.shape["ja"], mesh.shape["af"]),
        ("y", "xh", "c", "z", "xl"),
    )
    in_specs = (P(("y", "xh", "c", "z"), "xl"), P())
    out_specs = P("xl", ("y", "xh", "c"), "z")
    return jax.shard_map(
        per_device, mesh=torus, in_specs=in_specs, out_specs=out_specs, check_vma=False
    )
```

```python
import jax
import jax.numpy as jnp
from jax import lax
from jax.experimental import pallas as pl
from jax.experimental.pallas import tpu as pltpu
from jax.sharding import Mesh
from jax.sharding import PartitionSpec as P


KS = 8
ROWS = 16
SIDE = ("y", "xh")
F8 = jnp.float8_e4m3fn
PLACES = {4: (0, 0), 3: (1, 0), 5: (3, 0), 2: (2, 0), 6: (0, 1), 1: (1, 1), 7: (3, 1), 0: (2, 1)}
Y_STEPS = (0, 1, 3, 2)


def broadcast_all(array, axis):
    size = lax.axis_size(axis)
    return lax.all_to_all(
        jnp.broadcast_to(array[None], (size, *array.shape)), axis, 0, 0, tiled=True
    )


def to_planes(array):
    pairs = []
    for y in range(4):
        for xh in range(2):
            for c in range(2):
                for z in range(8):
                    plane = 2 * y + xh
                    dy, dx = PLACES[(z - plane) % 8]
                    there = (((y + dy) % 4) * 2 + (xh + dx) % 2) * 2 + c
                    pairs.append((((y * 2 + xh) * 2 + c) * 8 + z, there * 8 + plane))
    return lax.ppermute(array, ("y", "xh", "c", "z"), pairs)


def swap(array, axis, bit=1):
    return lax.ppermute(array, axis, [(n, n ^ bit) for n in range(lax.axis_size(axis))])


def spread(array, axis, bit, root):
    other = swap(array, axis, bit)
    return jnp.where((lax.axis_index(axis) & bit) == (root & bit), array, other)


def bits(words, bit):
    mask = jnp.int8((1 << bit) - (1 << 8 if bit == 7 else 0))
    return jnp.where((words & mask) != 0, jnp.full(words.shape, 1, F8), jnp.full(words.shape, 0, F8))


def pieces(words):
    return [(lax.shift_right_logical(words, s) if s else words).astype(jnp.int8) for s in range(0, 32, 8)]


def popcounts(words):
    return lax.population_count(words).astype(jnp.float32)


def place_j(mine, theirs, jbuf):
    core, plane, y, xh = (lax.axis_index(a) for a in ("c", "z", "y", "xh"))
    for slot in range(8):
        y_from = y - Y_STEPS[slot // 2]
        dy = (y_from - plane // 2) & 3
        dx = (xh + slot + plane) & 1
        dz = jnp.int32(0)
        for step, (at_y, at_x) in PLACES.items():
            dz = jnp.where((dy == at_y) & (dx == at_x), step, dz)
        row = ((plane + dz) & 7) * ROWS
        own = pl.multiple_of(core * 128 + row, ROWS)
        other = pl.multiple_of((1 - core) * 128 + row, ROWS)
        jbuf[pl.ds(own, ROWS), :] = mine[slot * ROWS : (slot + 1) * ROWS, :]
        jbuf[pl.ds(other, ROWS), :] = theirs[slot * ROWS : (slot + 1) * ROWS, :]


def counts_into(acc, base, i_ref, j_ref, thirds):
    i_parts, j_parts, k_parts = pieces(i_ref[...]), pieces(j_ref[...]), pieces(thirds)
    for i_part, j_part, k_part in zip(i_parts, j_parts, k_parts):
        pairs = jnp.concatenate([i_part & k_part[t : t + 1] for t in range(4)], axis=0)
        part = lax.dot_general(
            jnp.concatenate([bits(pairs, b) for b in range(8)], axis=1),
            jnp.concatenate([bits(j_part, b) for b in range(8)], axis=1),
            (((1,), (1,)), ((), ())),
            preferred_element_type=jnp.float32,
        )
        acc[...] = part if base is None else base[...] + part
        base = acc


def ones_of(i_ref, j_ref):
    ones_i = jnp.sum(popcounts(i_ref[...]), axis=1, keepdims=True)
    j_counts = popcounts(j_ref[...]).astype(jnp.bfloat16)
    ones_j = lax.dot_general(
        jnp.ones((8, j_counts.shape[1]), jnp.bfloat16),
        j_counts,
        (((1,), (1,)), ((), ())),
        preferred_element_type=jnp.float32,
    )[0:1]
    return ones_i + ones_j


def own_half(iw, mine, theirs, thirds, acc, ones, jbuf):
    place_j(mine, theirs, jbuf)
    counts_into(acc, None, iw, jbuf, thirds[0:4])
    ones[...] = ones_of(iw, jbuf)


def other_half(iw, mine, theirs, thirds, base, ones, out, jbuf, acc):
    place_j(mine, theirs, jbuf)
    counts_into(acc, base, iw, jbuf, thirds[4:8])
    ones_k = jnp.sum(popcounts(thirds[0:4]) + popcounts(thirds[4:8]), axis=1, keepdims=True)
    ones_ij = ones[...] + ones_of(iw, jbuf) + 1.0
    for t in range(4):
        out[t] = 3.0 * acc[t * 128 : (t + 1) * 128, :] / (ones_ij + ones_k[t : t + 1])


def on_core(kernel, operands, outs, scratch):
    operands = [pltpu.with_memory_space_constraint(a, pltpu.VMEM) for a in operands]
    return pl.pallas_call(
        kernel,
        out_shape=outs,
        in_specs=[VM] * len(operands),
        out_specs=jax.tree.map(lambda _: VM, outs),
        scratch_shapes=[pltpu.VMEM(*s) for s in scratch],
        cost_estimate=COST,
    )(*operands)


VM = pl.BlockSpec(memory_space=pltpu.VMEM)
COST = pl.CostEstimate(flops=2 * 512 * 256 * 16384, bytes_accessed=2**21, transcendentals=0)


def turn(array, step):
    return lax.ppermute(array, "y", [(n, (n + step) % 4) for n in range(4)])


def per_device(alleles, section):
    words = alleles.shape[1]
    half = lax.axis_index("xl")
    row = section[0] * KS
    ia_s = row // 128
    moved = to_planes(alleles)
    iwords = broadcast_all(alleles, "z").reshape(128, words)
    pair = jnp.concatenate([moved, swap(moved, "xh")], axis=0)
    slab = lax.dynamic_slice_in_dim(iwords, lax.rem(row, 128), KS, 0).reshape(1, 2, 4, words)
    slab = jnp.broadcast_to(slab, (8, 2, 4, words)).reshape(16, 4, words)
    came = lax.all_to_all(slab, (*SIDE, "xl"), 0, 0, tiled=True).reshape(8, 2, 4, words)
    came = lax.dynamic_index_in_dim(came, ia_s // 2, 0, keepdims=False)
    k_own = lax.dynamic_index_in_dim(came, half, 0, keepdims=False)
    k_other = lax.dynamic_index_in_dim(came, 1 - half, 0, keepdims=False)
    thirds = jnp.concatenate([k_own, k_other], axis=0)
    iwords_x = swap(iwords, "xl")
    turns = [turn(pair, d) for d in Y_STEPS[1:]]
    mine = jnp.concatenate([pair, *turns], axis=0)
    thirds = spread(thirds, "c", 1, lax.rem(ia_s, 2))
    mine_x = swap(mine, "xl")
    theirs = swap(mine, "c")
    theirs_x = swap(mine_x, "c")
    j_words = ((256, words), jnp.int32)
    counts, ones = on_core(
        own_half,
        [iwords, mine, theirs, thirds],
        (pltpu.VMEM((512, 256), jnp.float32), pltpu.VMEM((128, 256), jnp.float32)),
        [j_words],
    )
    return on_core(
        other_half,
        [iwords_x, mine_x, theirs_x, thirds, counts, ones],
        jax.ShapeDtypeStruct((4, 128, 256), jnp.float32),
        [j_words, ((512, 256), jnp.float32)],
    )


def solution(mesh):
    torus = Mesh(
        mesh.devices.reshape(4, 2, 2, mesh.shape["ja"], mesh.shape["af"]),
        ("y", "xh", "c", "z", "xl"),
    )
    in_specs = (P(("y", "xh", "c", "z"), "xl"), P())
    out_specs = P("xl", ("y", "xh", "c"), "z")


    return jax.shard_map(
        per_device, mesh=torus, in_specs=in_specs, out_specs=out_specs, check_vma=False
    )
```

```python
import jax
import jax.numpy as jnp
from jax import lax
from jax.experimental import pallas as pl
from jax.experimental.pallas import tpu as pltpu
from jax.sharding import Mesh
from jax.sharding import PartitionSpec as P


KS = 8
ROWS = 16
SIDE = ("y", "xh")
F8 = jnp.float8_e4m3fn
PLACES = {4: (0, 0), 3: (1, 0), 5: (3, 0), 2: (2, 0), 6: (0, 1), 1: (1, 1), 7: (3, 1), 0: (2, 1)}
Y_STEPS = (0, 1, 3, 2)


def broadcast_all(array, axis):
    size = lax.axis_size(axis)
    return lax.all_to_all(
        jnp.broadcast_to(array[None], (size, *array.shape)), axis, 0, 0, tiled=True
    )


def to_planes(array):
    pairs = []
    for y in range(4):
        for xh in range(2):
            for c in range(2):
                for z in range(8):
                    plane = 2 * y + xh
                    dy, dx = PLACES[(z - plane) % 8]
                    there = (((y + dy) % 4) * 2 + (xh + dx) % 2) * 2 + c
                    pairs.append((((y * 2 + xh) * 2 + c) * 8 + z, there * 8 + plane))
    return lax.ppermute(array, ("y", "xh", "c", "z"), pairs)


def swap(array, axis, bit=1):
    return lax.ppermute(array, axis, [(n, n ^ bit) for n in range(lax.axis_size(axis))])


def cross(array):
    return lax.ppermute(array, ("xh", "xl"), [(n, 3 - n) for n in range(4)])


def spread(array, axis, bit, root):
    other = swap(array, axis, bit)
    return jnp.where((lax.axis_index(axis) & bit) == (root & bit), array, other)


def bits(words, bit):
    mask = jnp.int8((1 << bit) - (1 << 8 if bit == 7 else 0))
    return jnp.where((words & mask) != 0, jnp.full(words.shape, 1, F8), jnp.full(words.shape, 0, F8))


def pieces(words):
    return [(lax.shift_right_logical(words, s) if s else words).astype(jnp.int8) for s in range(0, 32, 8)]


def popcounts(words):
    return lax.population_count(words).astype(jnp.float32)


def place_j(mine, theirs, jbuf, half):
    core, plane, y, xh = (lax.axis_index(a) for a in ("c", "z", "y", "xh"))
    for slot in range(8):
        y_from = y - Y_STEPS[slot // 2]
        dy = (y_from - plane // 2) & 3
        dx = (xh + slot + plane) & 1
        dz = jnp.int32(0)
        for step, (at_y, at_x) in PLACES.items():
            dz = jnp.where((dy == at_y) & (dx == at_x), step, dz)
        row = ((plane + dz) & 7) * ROWS
        own = pl.multiple_of(core * 128 + row, ROWS)
        other = pl.multiple_of((1 - core) * 128 + row, ROWS)
        source = slice((slot // 2 * 4 + half * 2 + slot % 2) * ROWS, (slot // 2 * 4 + half * 2 + slot % 2 + 1) * ROWS)
        jbuf[pl.ds(own, ROWS), :] = mine[source, :]
        jbuf[pl.ds(other, ROWS), :] = theirs[source, :]


def counts_into(acc, base, i_ref, j_ref, thirds):
    i_parts, j_parts, k_parts = pieces(i_ref[...]), pieces(j_ref[...]), pieces(thirds)
    for i_part, j_part, k_part in zip(i_parts, j_parts, k_parts):
        pairs = jnp.concatenate([i_part & k_part[t : t + 1] for t in range(4)], axis=0)
        part = lax.dot_general(
            jnp.concatenate([bits(pairs, b) for b in range(8)], axis=1),
            jnp.concatenate([bits(j_part, b) for b in range(8)], axis=1),
            (((1,), (1,)), ((), ())),
            preferred_element_type=jnp.float32,
        )
        acc[...] = part if base is None else base[...] + part
        base = acc


def ones_of(i_ref, j_ref):
    ones_i = jnp.sum(popcounts(i_ref[...]), axis=1, keepdims=True)
    j_counts = popcounts(j_ref[...]).astype(jnp.bfloat16)
    ones_j = lax.dot_general(
        jnp.ones((8, j_counts.shape[1]), jnp.bfloat16),
        j_counts,
        (((1,), (1,)), ((), ())),
        preferred_element_type=jnp.float32,
    )[0:1]
    return ones_i + ones_j


def metric(iw, iw_x, mine, theirs, thirds, out, jbuf, jbuf_x, acc):
    place_j(mine, theirs, jbuf, 0)
    place_j(mine, theirs, jbuf_x, 1)
    counts_into(acc, None, iw, jbuf, thirds[0:4])
    counts_into(acc, acc, iw_x, jbuf_x, thirds[4:8])
    ones_k = jnp.sum(popcounts(thirds[0:4]) + popcounts(thirds[4:8]), axis=1, keepdims=True)
    ones_ij = ones_of(iw, jbuf) + ones_of(iw_x, jbuf_x) + 1.0
    for t in range(4):
        out[t] = 3.0 * acc[t * 128 : (t + 1) * 128, :] / (ones_ij + ones_k[t : t + 1])


def on_core(kernel, operands, outs, scratch):
    operands = [pltpu.with_memory_space_constraint(a, pltpu.VMEM) for a in operands]
    return pl.pallas_call(
        kernel,
        out_shape=outs,
        in_specs=[VM] * len(operands),
        out_specs=jax.tree.map(lambda _: VM, outs),
        scratch_shapes=[pltpu.VMEM(*s) for s in scratch],
        cost_estimate=COST,
    )(*operands)


VM = pl.BlockSpec(memory_space=pltpu.VMEM)
COST = pl.CostEstimate(flops=2 * 512 * 256 * 32768, bytes_accessed=2**21, transcendentals=0)


def turn(array, step):
    return lax.ppermute(array, "y", [(n, (n + step) % 4) for n in range(4)])


def per_device(alleles, section):
    words = alleles.shape[1]
    half = lax.axis_index("xl")
    row = section[0] * KS
    ia_s = row // 128
    moved = to_planes(alleles)
    iwords = broadcast_all(alleles, "z").reshape(128, words)
    quad = jnp.concatenate(
        [moved, swap(moved, "xh"), swap(moved, "xl"), cross(moved)],
        axis=0,
    )
    slab = lax.dynamic_slice_in_dim(iwords, lax.rem(row, 128), KS, 0)
    slab = spread(slab, "c", 1, lax.rem(ia_s, 2))
    slab = jnp.broadcast_to(slab.reshape(1, 2, 4, words), (8, 2, 4, words)).reshape(16, 4, words)
    came = lax.all_to_all(slab, (*SIDE, "xl"), 0, 0, tiled=True).reshape(8, 2, 4, words)
    came = lax.dynamic_index_in_dim(came, ia_s // 2, 0, keepdims=False)
    k_own = lax.dynamic_index_in_dim(came, half, 0, keepdims=False)
    k_other = lax.dynamic_index_in_dim(came, 1 - half, 0, keepdims=False)
    thirds = jnp.concatenate([k_own, k_other], axis=0)
    iwords_x = swap(iwords, "xl")
    turns = [turn(quad, d) for d in Y_STEPS[1:]]
    mine = jnp.concatenate([quad, *turns], axis=0)
    theirs = swap(mine, "c")
    j_words = ((256, words), jnp.int32)
    return on_core(
        metric,
        [iwords, iwords_x, mine, theirs, thirds],
        jax.ShapeDtypeStruct((4, 128, 256), jnp.float32),
        [j_words, j_words, ((512, 256), jnp.float32)],
    )


def solution(mesh):
    torus = Mesh(
        mesh.devices.reshape(4, 2, 2, mesh.shape["ja"], mesh.shape["af"]),
        ("y", "xh", "c", "z", "xl"),
    )
    in_specs = (P(("y", "xh", "c", "z"), "xl"), P())
    out_specs = P("xl", ("y", "xh", "c"), "z")


    return jax.shard_map(per_device, mesh=torus, in_specs=in_specs, out_specs=out_specs, check_vma=False)
```

```python
import jax
import jax.numpy as jnp
from jax import lax
from jax.experimental import pallas as pl
from jax.experimental.pallas import tpu as pltpu
from jax.sharding import Mesh
from jax.sharding import PartitionSpec as P


KS = 8
ROWS = 16
SIDE = ("y", "xh")
F8 = jnp.float8_e4m3fn
PLACES = {4: (0, 0), 3: (1, 0), 5: (3, 0), 2: (2, 0), 6: (0, 1), 1: (1, 1), 7: (3, 1), 0: (2, 1)}
Y_STEPS = (0, 1, 3, 2)


def broadcast_all(array, axis):
    size = lax.axis_size(axis)
    return lax.all_to_all(
        jnp.broadcast_to(array[None], (size, *array.shape)), axis, 0, 0, tiled=True
    )


def to_planes(array):
    pairs = []
    for y in range(4):
        for xh in range(2):
            for c in range(2):
                for z in range(8):
                    plane = 2 * y + xh
                    dy, dx = PLACES[(z - plane) % 8]
                    there = (((y + dy) % 4) * 2 + (xh + dx) % 2) * 2 + c
                    pairs.append((((y * 2 + xh) * 2 + c) * 8 + z, there * 8 + plane))
    return lax.ppermute(array, ("y", "xh", "c", "z"), pairs)


def swap(array, axis, bit=1):
    return lax.ppermute(array, axis, [(n, n ^ bit) for n in range(lax.axis_size(axis))])


def cross(array):
    return lax.ppermute(array, ("xh", "xl"), [(n, 3 - n) for n in range(4)])


def spread(array, axis, bit, root):
    other = swap(array, axis, bit)
    return jnp.where((lax.axis_index(axis) & bit) == (root & bit), array, other)


def bits(words, bit):
    mask = jnp.int8((1 << bit) - (1 << 8 if bit == 7 else 0))
    return jnp.where((words & mask) != 0, jnp.full(words.shape, 1, F8), jnp.full(words.shape, 0, F8))


def pieces(words):
    return [(lax.shift_right_logical(words, s) if s else words).astype(jnp.int8) for s in range(0, 32, 8)]


def popcounts(words):
    return lax.population_count(words).astype(jnp.float32)


def place_j(mine, theirs, jbuf, half):
    core, plane, y, xh = (lax.axis_index(a) for a in ("c", "z", "y", "xh"))
    for slot in range(8):
        y_from = y - Y_STEPS[slot // 2]
        dy = (y_from - plane // 2) & 3
        dx = (xh + slot + plane) & 1
        dz = jnp.int32(0)
        for step, (at_y, at_x) in PLACES.items():
            dz = jnp.where((dy == at_y) & (dx == at_x), step, dz)
        row = ((plane + dz) & 7) * ROWS
        own = pl.multiple_of(core * 128 + row, ROWS)
        other = pl.multiple_of((1 - core) * 128 + row, ROWS)
        source = slice((slot // 2 * 4 + half * 2 + slot % 2) * ROWS, (slot // 2 * 4 + half * 2 + slot % 2 + 1) * ROWS)
        jbuf[pl.ds(own, ROWS), :] = mine[source, :]
        jbuf[pl.ds(other, ROWS), :] = theirs[source, :]


def planes(words):
    return jnp.concatenate([bits(words, b) for b in range(8)], axis=1)


def product(i_part, j_planes, k_part):
    pairs = jnp.concatenate([i_part & k_part[t : t + 1] for t in range(k_part.shape[0])], axis=0)
    return lax.dot_general(
        planes(pairs), j_planes, (((1,), (1,)), ((), ())), preferred_element_type=jnp.float32
    )


def counts_into(acc, base, i_ref, j_ref, thirds, keep=0):
    parts = list(zip(pieces(i_ref[...]), pieces(j_ref[...]), pieces(thirds)))
    for i_part, j_part, k_part in parts[: 4 - keep]:
        part = product(i_part, planes(j_part), k_part)
        acc[...] = part if base is None else base[...] + part
        base = acc
    return [(i_part, planes(j_part), k_part) for i_part, j_part, k_part in parts[4 - keep :]]


def ones_of(i_ref, j_ref):
    ones_i = jnp.sum(popcounts(i_ref[...]), axis=1, keepdims=True)
    j_counts = popcounts(j_ref[...]).astype(jnp.bfloat16)
    ones_j = lax.dot_general(
        jnp.ones((8, j_counts.shape[1]), jnp.bfloat16),
        j_counts,
        (((1,), (1,)), ((), ())),
        preferred_element_type=jnp.float32,
    )[0:1]
    return ones_i + ones_j


def metric(section, iw, iw_x, mine, theirs, came, out, jbuf, jbuf_x, acc, rows, sems):
    place_j(mine, theirs, jbuf, 0)
    place_j(mine, theirs, jbuf_x, 1)
    half = lax.axis_index("xl")
    root = ((section[0] * KS) // 256) * 2
    k_own, k_other = came[root + half], came[root + 1 - half]
    ones_k = jnp.sum(popcounts(k_own) + popcounts(k_other), axis=1, keepdims=True)
    ones_ij = ones_of(iw, jbuf) + ones_of(iw_x, jbuf_x) + 1.0
    counts_into(acc, None, iw, jbuf, k_own)
    tail = counts_into(acc, acc, iw_x, jbuf_x, k_other, keep=1)
    copies = [pltpu.make_async_copy(rows.at[t], out.at[t], sems.at[t]) for t in range(4)]
    for i_part, j_planes, k_part in tail:
        for pair in range(0, 4, 2):
            part = product(i_part, j_planes, k_part[pair : pair + 2])
            for t in (pair, pair + 1):
                counts = acc[t * 128 : (t + 1) * 128, :] + part[(t - pair) * 128 : (t - pair + 1) * 128]
                rows[t] = 3.0 * counts / (ones_ij + ones_k[t : t + 1])
                copies[t].start()
    for copy in copies:
        copy.wait()


def on_core(kernel, operands, section, outs, scratch):
    operands = [pltpu.with_memory_space_constraint(a, pltpu.VMEM) for a in operands]
    return pl.pallas_call(
        kernel,
        out_shape=outs,
        in_specs=[pl.BlockSpec(memory_space=pltpu.SMEM)] + [VM] * len(operands),
        out_specs=pl.BlockSpec(memory_space=pl.ANY),
        scratch_shapes=scratch,
        cost_estimate=COST,
    )(section, *operands)


VM = pl.BlockSpec(memory_space=pltpu.VMEM)
COST = pl.CostEstimate(flops=2 * 512 * 256 * 32768, bytes_accessed=2**21, transcendentals=0)


def turn(array, step):
    return lax.ppermute(array, "y", [(n, (n + step) % 4) for n in range(4)])


def per_device(alleles, section):
    words = alleles.shape[1]
    row = section[0] * KS
    ia_s = row // 128
    moved = to_planes(alleles)
    iwords = broadcast_all(alleles, "z").reshape(128, words)
    quad = jnp.concatenate(
        [moved, swap(moved, "xh"), swap(moved, "xl"), cross(moved)],
        axis=0,
    )
    slab = lax.dynamic_slice_in_dim(iwords, lax.rem(row, 128), KS, 0)
    slab = spread(slab, "c", 1, lax.rem(ia_s, 2))
    slab = jnp.broadcast_to(slab.reshape(1, 2, 4, words), (8, 2, 4, words)).reshape(16, 4, words)
    came = lax.all_to_all(slab, (*SIDE, "xl"), 0, 0, tiled=True)
    iwords_x = swap(iwords, "xl")
    turns = [turn(quad, d) for d in Y_STEPS[1:]]
    mine = jnp.concatenate([quad, *turns], axis=0)
    theirs = swap(mine, "c")
    j_words = pltpu.VMEM((256, words), jnp.int32)
    return on_core(
        metric,
        [iwords, iwords_x, mine, theirs, came],
        section,
        jax.ShapeDtypeStruct((4, 128, 256), jnp.float32),
        [
            j_words,
            j_words,
            pltpu.VMEM((512, 256), jnp.float32),
            pltpu.VMEM((4, 128, 256), jnp.float32),
            pltpu.SemaphoreType.DMA((4,)),
        ],
    )


def solution(mesh):
    torus = Mesh(
        mesh.devices.reshape(4, 2, 2, mesh.shape["ja"], mesh.shape["af"]),
        ("y", "xh", "c", "z", "xl"),
    )
    in_specs = (P(("y", "xh", "c", "z"), "xl"), P())
    out_specs = P("xl", ("y", "xh", "c"), "z")


    return jax.shard_map(per_device, mesh=torus, in_specs=in_specs, out_specs=out_specs, check_vma=False)
```
